32 devices in a mesh: seq: 2 (over x), tensor: 4 (over z), bucket: 4 (over y, core).
Axes of the slice: x: 2, y: 2, z: 4, core: 2. Of those that a mesh axis runs over, the one named last changes fastest.
Arguments:
- queries: bfloat16 [4, 1024, 3072], P('bucket', ('seq', 'tensor')), may hold values from -6 to 6
- keys: bfloat16 [4, 1024, 3072], P('bucket', ('seq', 'tensor')), may hold values from -6 to 6
- values: bfloat16 [4, 1024, 3072], P('bucket', ('seq', 'tensor')), may hold values from -6 to 6
- lengths: int32 [4], P('bucket'), may hold values from 256 to 1024, as said below
- out_weight: bfloat16 [3072, 3072], P(('seq', 'bucket'), 'tensor'), may hold values from -0.109375 to 0.109375
Outputs:
- projected: bfloat16 [4, 1024, 3072], P('bucket', ('seq', 'tensor'))
The draws below stay inside these ranges and needn't reach their ends.
Inputs may be any that keep to these rules, and one draw needn't show every extreme that they name: `lengths`: each bucket has 256 to 1024 live tokens, and at least one bucket has all 1024.
All inputs are finite; a program needn't handle non-finite values.
Results may differ from the reference program's by a relative error of at most 0.018.
Values may be sent and summed in bfloat16 or wider, within the bound.
A program may use at most 128 MiB of HBM per device.

```python
import jax
import jax.numpy as jnp
from jax import lax

D = 3072
HEADS = 24
HS = 128
LEN = 1024
BUCKETS = 4


def draw_queries(key, part):
    drawn = jax.random.normal(jax.random.fold_in(key, 1), (BUCKETS, LEN, D), jnp.float32)
    return jnp.clip(drawn, -6.0, 6.0).astype(jnp.bfloat16)


def draw_keys(key, part):
    drawn = jax.random.normal(jax.random.fold_in(key, 2), (BUCKETS, LEN, D), jnp.float32)
    return jnp.clip(drawn, -6.0, 6.0).astype(jnp.bfloat16)


def draw_lengths(key, part):
    drawn = jax.random.randint(jax.random.fold_in(key, 3), (BUCKETS,), LEN // 4, LEN + 1)
    fullest = jax.random.randint(jax.random.fold_in(key, 4), (), 0, BUCKETS)
    return jnp.where(jnp.arange(BUCKETS) == fullest, LEN, drawn).astype(jnp.int32)


def block_levels(rng, dims, pieces, low, top_value):
    level, own = 1.0, jax.random.fold_in(rng, 6)
    for position, parts in pieces:
        steps = jnp.exp(jax.random.uniform(jax.random.fold_in(own, position), (parts,), jnp.float32, low / len(pieces), top_value / len(pieces)))
        level = level * jnp.repeat(steps, dims[position] // parts).reshape([-1 if axis == position else 1 for axis in range(len(dims))])
    return level


def gaussian(rng, extent, width, limit, cuts=(), held_as=jnp.bfloat16):
    result = jax.random.normal(rng, extent, jnp.float32) * width
    if len(cuts) > 0:
        result = block_levels(rng, extent, cuts, -0.22, 0.18) * result
    return jnp.clip(result, min=-limit, max=limit).astype(held_as)


def setup_inputs(seed: int = 0) -> dict:
    key_list = jax.random.split(jax.random.key(seed), 6)
    queries = draw_queries(jax.random.fold_in(key_list[5], 71), 0)
    keys = draw_keys(jax.random.fold_in(key_list[5], 71), 0)
    values = gaussian(key_list[2], (BUCKETS, LEN, D), 1.0, 6.0, ((0, 4), (1, 8)))
    lengths = draw_lengths(jax.random.fold_in(key_list[5], 71), 0)
    out_weight = gaussian(key_list[4], (D, D), D ** -0.5, 0.109375, ((0, 8), (1, 4)))
    return {"queries": queries, "keys": keys, "values": values, "lengths": lengths, "out_weight": out_weight}


MASKED_SCORE = -1e30


def attend_head(query_head, key_head, value_head, usable):
    scores = jnp.dot(query_head, key_head.T, preferred_element_type=jnp.float32) * (HS ** -0.5)
    scores = jnp.where(usable[None, :], scores, MASKED_SCORE)
    row_peak = jnp.max(scores, axis=-1, keepdims=True)
    exponent = jnp.where(usable[None, :], jnp.exp(scores - row_peak), 0.0)
    numerator = jnp.dot(exponent.astype(jnp.bfloat16), value_head, preferred_element_type=jnp.float32)
    return numerator / jnp.sum(exponent, axis=-1, keepdims=True)


def reference(queries, keys, values, lengths, out_weight):
    def split_heads(array):
        return array.reshape(LEN, HEADS, HS).transpose(1, 0, 2)

    def one_bucket(inputs):
        bucket_q, bucket_k, bucket_v, live_len = inputs
        positions = jnp.arange(LEN, dtype=jnp.int32)
        usable = positions < live_len

        def one_head(trio):
            return attend_head(trio[0], trio[1], trio[2], usable)

        attended = lax.map(one_head, (split_heads(bucket_q), split_heads(bucket_k), split_heads(bucket_v)))
        mixed = attended.transpose(1, 0, 2).reshape(LEN, D)
        mixed = jnp.where(usable[:, None], mixed, 0.0).astype(jnp.bfloat16)
        return jnp.dot(mixed, out_weight, preferred_element_type=jnp.float32).astype(jnp.bfloat16)

    return lax.map(one_bucket, (queries, keys, values, lengths))
```

```python
import functools
import math

import jax
import jax.numpy as jnp
from jax import lax
from jax.experimental import pallas as pl
from jax.experimental.pallas import tpu as pltpu
from jax.sharding import PartitionSpec as P

HS = 128


MASKED_SCORE = -1e30


def shards(queries, keys, values, lengths, out_weight):
    tok_rows = queries.shape[1]
    n_tensor = lax.axis_size("tensor")
    tensor_index = lax.axis_index("tensor")
    live_len = lengths[0]
    local_q, local_k, local_v = (
        lax.all_to_all(queries[0], "seq", split_axis=1, concat_axis=0, tiled=True),
        lax.all_to_all(keys[0], "seq", split_axis=1, concat_axis=0, tiled=True),
        lax.all_to_all(values[0], "seq", split_axis=1, concat_axis=0, tiled=True),
    )
    row_count, col_count = local_q.shape
    head_count = col_count // HS
    query_heads = local_q.reshape(row_count, head_count, HS)

    def spots(first_row, total_rows):
        index_row = first_row + jnp.arange(total_rows, dtype=jnp.int32)
        owner = index_row // row_count
        within = index_row % row_count
        return (within // tok_rows * n_tensor + owner) * tok_rows + within % tok_rows

    query_usable = spots(tensor_index * row_count, row_count) < live_len
    initial = (
        jnp.full((row_count, head_count), MASKED_SCORE, jnp.float32),
        jnp.zeros((row_count, head_count), jnp.float32),
        jnp.zeros((row_count, head_count, HS), jnp.float32),
    )
    carried = initial
    first_row = jnp.int32(0)
    key_rows = lax.all_gather(local_k, "tensor", axis=0, tiled=True)
    value_rows = lax.all_gather(local_v, "tensor", axis=0, tiled=True)
    for offset in range(key_rows.shape[0] // row_count):
        row_peak, row_sum, accumulated = carried
        key_tile = key_rows[offset * row_count : (offset + 1) * row_count].reshape(
            row_count, head_count, HS
        )
        value_tile = value_rows[offset * row_count : (offset + 1) * row_count].reshape(
            row_count, head_count, HS
        )
        key_usable = spots(first_row + offset * row_count, row_count) < live_len
        scores = jnp.einsum(
            "qhd,khd->qhk", query_heads, key_tile, preferred_element_type=jnp.float32
        ) * HS ** (-0.5)
        scores = jnp.where(key_usable[None, None, :], scores, MASKED_SCORE)
        peak_new = jnp.maximum(row_peak, jnp.max(scores, axis=-1))
        exponent = jnp.where(key_usable[None, None, :], jnp.exp(scores - peak_new[..., None]), 0.0)
        rescale = jnp.exp(row_peak - peak_new)
        accumulated = accumulated * rescale[..., None] + jnp.einsum(
            "qhk,khd->qhd",
            exponent.astype(jnp.bfloat16),
            value_tile,
            preferred_element_type=jnp.float32,
        )
        carried = (peak_new, row_sum * rescale + jnp.sum(exponent, axis=-1), accumulated)
    row_peak, row_sum, accumulated = carried
    attended = accumulated / row_sum[..., None]
    mixed = jnp.where(query_usable[:, None], attended.reshape(row_count, col_count), 0.0).astype(
        jnp.bfloat16
    )
    restored = lax.all_to_all(mixed, "seq", split_axis=0, concat_axis=1, tiled=True)
    wide_weight = lax.all_gather(out_weight, "tensor", axis=1, tiled=True)
    summed = jnp.dot(
        restored,
        lax.all_gather(wide_weight, ("seq", "bucket"), axis=0, tiled=True),
        preferred_element_type=jnp.float32,
    )
    return summed.astype(jnp.bfloat16)[None]


def whole_kernel(
    axes, sizes, len_ref, q_ref, k_ref, v_ref, w_ref, out_ref,
    got, done, mixed, weight, part_out, part_in, own_part,
    qkv_send, qkv_recv, att_send, att_recv, up_send, down_send, line_recv,
    far_send, far_recv, near_send, near_recv, part_send, part_recv,
):
    n_seq, n_tensor, n_bucket = sizes
    s, t, b = lax.axis_index("seq"), lax.axis_index("tensor"), lax.axis_index("bucket")
    group = n_seq * n_tensor
    rows = q_ref.shape[1]
    width = q_ref.shape[2]
    heads = width // HS // group
    w_rows, w_cols = w_ref.shape
    block = n_seq * rows
    live = len_ref[0]

    def device(ds, dt, db):
        place = {"seq": ds, "tensor": dt, "bucket": db}
        return tuple(place[name] for name in axes)

    def remote(src, dst, send, recv, where):
        return pltpu.make_async_remote_copy(
            src_ref=src, dst_ref=dst, send_sem=send, recv_sem=recv,
            device_id=where, device_id_type=pl.DeviceIdType.MESH,
        )

    me = s * n_tensor + t
    streams = (q_ref, k_ref, v_ref)

    def spot(ds, dt):
        return pl.ds(pl.multiple_of((dt * n_seq + ds) * rows, rows), rows)

    def qkv_copy(h, j, step, peer, source):
        cols = pl.ds(pl.multiple_of((peer * heads + h) * HS, HS), HS)
        return remote(
            streams[j].at[0, :, cols],
            got.at[h, j, spot(source // n_tensor, source % n_tensor), :],
            qkv_send.at[h, j, step],
            qkv_recv.at[h, j, step],
            device(peer // n_tensor, peer % n_tensor, b),
        )

    def start_qkv(h):
        def body(step, carry):
            peer = (me + step) % group
            for j in range(3):
                qkv_copy(h, j, step, peer, me).start()
            return carry

        lax.fori_loop(1, group, body, 0)

    def piece(row_block, col_block):
        return weight.at[
            pl.ds(pl.multiple_of(row_block * w_rows, w_rows), w_rows),
            pl.ds(pl.multiple_of(col_block * w_cols, w_cols), w_cols),
        ]

    far, near = (b + 2) % 4, b + 1 - 2 * (b % 2)

    def up_copy(p):
        return remote(piece(b, p), piece(b, p), up_send.at[p], line_recv.at[p], device(s, t + 1, b))

    def down_copy(p):
        return remote(piece(b, p), piece(b, p), down_send.at[p], line_recv.at[p], device(s, t - 1, b))

    def far_copy(p, row_block):
        return remote(piece(row_block, p), piece(row_block, p), far_send.at[p], far_recv.at[p], device(s, t, far))

    def near_copy(k, p, row_block):
        return remote(
            piece(row_block, p), piece(row_block, p), near_send.at[k, p], near_recv.at[k, p], device(s, t, near)
        )

    def spread(p):
        far_copy(p, b).start()
        near_copy(0, p, b).start()

    def relay(k):
        @pl.when(t >= k)
        def _():
            up_copy(t - k).wait_recv()

            @pl.when(t < n_tensor - 1)
            def _():
                up_copy(t - k).start()

            spread(t - k)

        @pl.when(t + k < n_tensor)
        def _():
            down_copy(t + k).wait_recv()

            @pl.when(t > 0)
            def _():
                down_copy(t + k).start()

            spread(t + k)

    start_qkv(0)
    weight[
        pl.ds(pl.multiple_of(b * w_rows, w_rows), w_rows),
        pl.ds(pl.multiple_of(t * w_cols, w_cols), w_cols),
    ] = w_ref[...]
    spread(t)
    for h in range(1, heads):
        start_qkv(h)

    @pl.when(t < n_tensor - 1)
    def _():
        up_copy(t).start()

    @pl.when(t > 0)
    def _():
        down_copy(t).start()

    for h in range(heads):
        cols = pl.ds(pl.multiple_of((me * heads + h) * HS, HS), HS)
        for j in range(3):
            got[h, j, spot(s, t), :] = streams[j][0, :, cols]

    total = group * rows
    index = lax.broadcasted_iota(jnp.int32, (1, total), 1)
    token = (index % block // rows * n_tensor + index // block) * rows + index % rows
    usable = token < live
    row_index = lax.broadcasted_iota(jnp.int32, (block, 1), 0)
    factor = HS ** (-0.5) * math.log2(math.e)

    def att_copy(h, step, target, source):
        here = pl.ds(pl.multiple_of(target * block, block), block)
        cols = pl.ds(pl.multiple_of((source * heads + h) * HS, HS), HS)
        return remote(
            done.at[h, here, :], mixed.at[:, cols], att_send.at[h, step], att_recv.at[h, step], device(s, target, b)
        )

    def attend(h, target):
        here = pl.ds(pl.multiple_of(target * block, block), block)
        scores = lax.dot_general(
            got[h, 0, here, :], got[h, 1], (((1,), (1,)), ((), ())), preferred_element_type=jnp.float32
        )
        scores = jnp.where(usable, scores, MASKED_SCORE)
        peak = jnp.max(scores, axis=-1, keepdims=True)
        expo = jnp.exp2((scores - peak) * factor)
        denominator = jnp.sum(expo, axis=-1, keepdims=True)
        result = jnp.dot(expo.astype(jnp.bfloat16), got[h, 2], preferred_element_type=jnp.float32) / denominator
        own_token = (row_index // rows * n_tensor + target) * rows + row_index % rows
        return jnp.where(own_token < live, result, 0.0).astype(jnp.bfloat16)

    for h in range(heads):
        def arrive(step, carry):
            source = (me + group - step) % group
            for j in range(3):
                qkv_copy(h, j, step, me, source).wait_recv()
            return carry

        lax.fori_loop(1, group, arrive, 0)

        def one(step, carry):
            target = (t + step) % n_tensor
            here = pl.ds(pl.multiple_of(target * block, block), block)
            done[h, here, :] = attend(h, target)
            att_copy(h, step, target, t).start()
            return carry

        lax.fori_loop(1, n_tensor, one, 0)
        mixed[:, pl.ds(pl.multiple_of((t * heads + h) * HS, HS), HS)] = attend(h, t)
        if h + 1 < n_tensor:
            relay(h + 1)
    for k in range(heads + 1, n_tensor):
        relay(k)

    for p in range(n_tensor):
        far_copy(p, far).wait_recv()
        near_copy(1, p, far).start()
    for p in range(n_tensor):
        near_copy(0, p, near).wait_recv()
        near_copy(1, p, (near + 2) % 4).wait_recv()
    for h in range(heads):
        def back(step, carry):
            att_copy(h, step, t, (t + n_tensor - step) % n_tensor).wait_recv()
            return carry

        lax.fori_loop(1, n_tensor, back, 0)

    def part_copy(p):
        cut = slice(p * w_cols, (p + 1) * w_cols)
        return remote(
            part_out.at[:, cut], part_in.at[:, cut], part_send.at[p], part_recv.at[p], device(1 - s, t, b)
        )

    for p in range(n_tensor):
        cut = slice(p * w_cols, (p + 1) * w_cols)
        summed = jnp.dot(mixed[...], weight[:, cut], preferred_element_type=jnp.float32)
        first, second = summed[:rows], summed[rows:]
        part_out[:, cut] = jnp.where(s == 0, second, first).astype(jnp.bfloat16)
        part_copy(p).start()
        own_part[:, cut] = jnp.where(s == 0, first, second)
    for p in range(n_tensor):
        cut = slice(p * w_cols, (p + 1) * w_cols)
        part_copy(p).wait_recv()
        out_ref[0, :, cut] = (own_part[:, cut] + part_in[:, cut].astype(jnp.float32)).astype(jnp.bfloat16)

    for h in range(heads):
        def sent(step, carry):
            peer = (me + step) % group
            for j in range(3):
                qkv_copy(h, j, step, peer, me).wait_send()
            return carry

        lax.fori_loop(1, group, sent, 0)

        def att_sent(step, carry):
            att_copy(h, step, (t + step) % n_tensor, t).wait_send()
            return carry

        lax.fori_loop(1, n_tensor, att_sent, 0)
    for k in range(n_tensor):
        @pl.when((t >= k) & (t < n_tensor - 1))
        def _():
            up_copy(t - k).wait_send()

        @pl.when((t + k < n_tensor) & (t > 0))
        def _():
            down_copy(t + k).wait_send()

    for p in range(n_tensor):
        far_copy(p, b).wait_send()
        near_copy(0, p, b).wait_send()
        near_copy(1, p, far).wait_send()
        part_copy(p).wait_send()


def fused(axes, sizes, queries, keys, values, lengths, out_weight):
    n_seq, n_tensor, n_bucket = sizes
    rows, width = queries.shape[1:]
    group = n_seq * n_tensor
    heads = width // HS // group
    total = group * rows
    half = width // n_seq
    vmem = pl.BlockSpec(memory_space=pltpu.VMEM)
    dma = pltpu.SemaphoreType.DMA
    return pl.pallas_call(
        functools.partial(whole_kernel, axes, sizes),
        out_shape=jax.ShapeDtypeStruct(queries.shape, queries.dtype),
        in_specs=[pl.BlockSpec(memory_space=pltpu.SMEM), vmem, vmem, vmem, vmem],
        out_specs=vmem,
        scratch_shapes=[
            pltpu.VMEM((heads, 3, total, HS), jnp.bfloat16),
            pltpu.VMEM((heads, total, HS), jnp.bfloat16),
            pltpu.VMEM((n_seq * rows, half), jnp.bfloat16),
            pltpu.VMEM((half, width), jnp.bfloat16),
            pltpu.VMEM((rows, width), jnp.bfloat16),
            pltpu.VMEM((rows, width), jnp.bfloat16),
            pltpu.VMEM((rows, width), jnp.float32),
            dma((heads, 3, group)),
            dma((heads, 3, group)),
            dma((heads, n_tensor)),
            dma((heads, n_tensor)),
            dma((n_tensor,)),
            dma((n_tensor,)),
            dma((n_tensor,)),
            dma((n_tensor,)),
            dma((n_tensor,)),
            dma((2, n_tensor)),
            dma((2, n_tensor)),
            dma((n_tensor,)),
            dma((n_tensor,)),
        ],
        compiler_params=pltpu.CompilerParams(has_side_effects=True, vmem_limit_bytes=56 * 1024 * 1024),
    )(lengths, queries, keys, values, out_weight)


def solution(mesh):
    in_specs = (
        P("bucket", ("seq", "tensor"), None),
        P("bucket", ("seq", "tensor"), None),
        P("bucket", ("seq", "tensor"), None),
        P("bucket"),
        P(("seq", "bucket"), "tensor"),
    )
    out_specs = P("bucket", ("seq", "tensor"), None)
    sizes = tuple(mesh.shape[name] for name in ("seq", "tensor", "bucket"))

    def step(queries, keys, values, lengths, out_weight):
        head_count = queries.shape[2] // HS
        fits = sizes[0] == 2 and sizes[1] == sizes[2] == 4 and head_count % (sizes[0] * sizes[1]) == 0
        if fits:
            return fused(mesh.axis_names, sizes, queries, keys, values, lengths, out_weight)
        return shards(queries, keys, values, lengths, out_weight)

    return jax.shard_map(step, mesh=mesh, in_specs=in_specs, out_specs=out_specs, check_vma=False)
```

```python
import functools
import math

import jax
import jax.numpy as jnp
from jax import lax
from jax.experimental import pallas as pl
from jax.experimental.pallas import tpu as pltpu
from jax.sharding import PartitionSpec as P

HS = 128


MASKED_SCORE = -1e30


def shards(queries, keys, values, lengths, out_weight):
    tok_rows = queries.shape[1]
    n_tensor = lax.axis_size("tensor")
    tensor_index = lax.axis_index("tensor")
    live_len = lengths[0]
    local_q, local_k, local_v = (
        lax.all_to_all(queries[0], "seq", split_axis=1, concat_axis=0, tiled=True),
        lax.all_to_all(keys[0], "seq", split_axis=1, concat_axis=0, tiled=True),
        lax.all_to_all(values[0], "seq", split_axis=1, concat_axis=0, tiled=True),
    )
    row_count, col_count = local_q.shape
    head_count = col_count // HS
    query_heads = local_q.reshape(row_count, head_count, HS)

    def spots(first_row, total_rows):
        index_row = first_row + jnp.arange(total_rows, dtype=jnp.int32)
        owner = index_row // row_count
        within = index_row % row_count
        return (within // tok_rows * n_tensor + owner) * tok_rows + within % tok_rows

    query_usable = spots(tensor_index * row_count, row_count) < live_len
    initial = (
        jnp.full((row_count, head_count), MASKED_SCORE, jnp.float32),
        jnp.zeros((row_count, head_count), jnp.float32),
        jnp.zeros((row_count, head_count, HS), jnp.float32),
    )
    carried = initial
    first_row = jnp.int32(0)
    key_rows = lax.all_gather(local_k, "tensor", axis=0, tiled=True)
    value_rows = lax.all_gather(local_v, "tensor", axis=0, tiled=True)
    for offset in range(key_rows.shape[0] // row_count):
        row_peak, row_sum, accumulated = carried
        key_tile = key_rows[offset * row_count : (offset + 1) * row_count].reshape(
            row_count, head_count, HS
        )
        value_tile = value_rows[offset * row_count : (offset + 1) * row_count].reshape(
            row_count, head_count, HS
        )
        key_usable = spots(first_row + offset * row_count, row_count) < live_len
        scores = jnp.einsum(
            "qhd,khd->qhk", query_heads, key_tile, preferred_element_type=jnp.float32
        ) * HS ** (-0.5)
        scores = jnp.where(key_usable[None, None, :], scores, MASKED_SCORE)
        peak_new = jnp.maximum(row_peak, jnp.max(scores, axis=-1))
        exponent = jnp.where(key_usable[None, None, :], jnp.exp(scores - peak_new[..., None]), 0.0)
        rescale = jnp.exp(row_peak - peak_new)
        accumulated = accumulated * rescale[..., None] + jnp.einsum(
            "qhk,khd->qhd",
            exponent.astype(jnp.bfloat16),
            value_tile,
            preferred_element_type=jnp.float32,
        )
        carried = (peak_new, row_sum * rescale + jnp.sum(exponent, axis=-1), accumulated)
    row_peak, row_sum, accumulated = carried
    attended = accumulated / row_sum[..., None]
    mixed = jnp.where(query_usable[:, None], attended.reshape(row_count, col_count), 0.0).astype(
        jnp.bfloat16
    )
    restored = lax.all_to_all(mixed, "seq", split_axis=0, concat_axis=1, tiled=True)
    wide_weight = lax.all_gather(out_weight, "tensor", axis=1, tiled=True)
    summed = jnp.dot(
        restored,
        lax.all_gather(wide_weight, ("seq", "bucket"), axis=0, tiled=True),
        preferred_element_type=jnp.float32,
    )
    return summed.astype(jnp.bfloat16)[None]


def whole_kernel(
    axes, sizes, len_ref, q_ref, k_ref, v_ref, w_ref, out_ref,
    got, done, mixed, weight, part_out, part_in, own_part,
    qkv_send, qkv_recv, att_send, att_recv, up_send, down_send, line_recv,
    far_send, far_recv, near_send, near_recv, part_send, part_recv, out_sem,
):
    n_seq, n_tensor, n_bucket = sizes
    s, t, b = lax.axis_index("seq"), lax.axis_index("tensor"), lax.axis_index("bucket")
    group = n_seq * n_tensor
    rows = q_ref.shape[1]
    width = q_ref.shape[2]
    heads = width // HS // group
    w_rows, w_cols = w_ref.shape
    block = n_seq * rows
    live = len_ref[0]

    def device(ds, dt, db):
        place = {"seq": ds, "tensor": dt, "bucket": db}
        return tuple(place[name] for name in axes)

    def remote(src, dst, send, recv, where):
        return pltpu.make_async_remote_copy(
            src_ref=src, dst_ref=dst, send_sem=send, recv_sem=recv,
            device_id=where, device_id_type=pl.DeviceIdType.MESH,
        )

    me = s * n_tensor + t
    streams = (q_ref, k_ref, v_ref)

    def spot(ds, dt):
        return pl.ds(pl.multiple_of((dt * n_seq + ds) * rows, rows), rows)

    def qkv_copy(h, j, step, peer, source):
        cols = pl.ds(pl.multiple_of((peer * heads + h) * HS, HS), HS)
        return remote(
            streams[j].at[0, :, cols],
            got.at[h, j, spot(source // n_tensor, source % n_tensor), :],
            qkv_send.at[h, j, step],
            qkv_recv.at[h, j, step],
            device(peer // n_tensor, peer % n_tensor, b),
        )

    def start_qkv(h):
        def body(step, carry):
            peer = (me + step) % group
            for j in range(3):
                qkv_copy(h, j, step, peer, me).start()
            return carry

        lax.fori_loop(1, group, body, 0)

    def piece(row_block, col_block):
        return weight.at[
            pl.ds(pl.multiple_of(row_block * w_rows, w_rows), w_rows),
            pl.ds(pl.multiple_of(col_block * w_cols, w_cols), w_cols),
        ]

    far, near = (b + 2) % 4, b + 1 - 2 * (b % 2)

    def up_copy(p):
        return remote(piece(b, p), piece(b, p), up_send.at[p], line_recv.at[p], device(s, t + 1, b))

    def down_copy(p):
        return remote(piece(b, p), piece(b, p), down_send.at[p], line_recv.at[p], device(s, t - 1, b))

    def far_copy(p, row_block):
        return remote(piece(row_block, p), piece(row_block, p), far_send.at[p], far_recv.at[p], device(s, t, far))

    def near_copy(k, p, row_block):
        return remote(
            piece(row_block, p), piece(row_block, p), near_send.at[k, p], near_recv.at[k, p], device(s, t, near)
        )

    def spread(p):
        far_copy(p, b).start()
        near_copy(0, p, b).start()

    def relay(k):
        @pl.when(t >= k)
        def _():
            up_copy(t - k).wait_recv()

            @pl.when(t < n_tensor - 1)
            def _():
                up_copy(t - k).start()

            spread(t - k)

        @pl.when(t + k < n_tensor)
        def _():
            down_copy(t + k).wait_recv()

            @pl.when(t > 0)
            def _():
                down_copy(t + k).start()

            spread(t + k)

    weight[
        pl.ds(pl.multiple_of(b * w_rows, w_rows), w_rows),
        pl.ds(pl.multiple_of(t * w_cols, w_cols), w_cols),
    ] = w_ref[...]

    @pl.when(t < n_tensor - 1)
    def _():
        up_copy(t).start()

    @pl.when(t > 0)
    def _():
        down_copy(t).start()

    start_qkv(0)
    spread(t)

    for h in range(heads):
        cols = pl.ds(pl.multiple_of((me * heads + h) * HS, HS), HS)
        for j in range(3):
            got[h, j, spot(s, t), :] = streams[j][0, :, cols]

    total = group * rows
    index = lax.broadcasted_iota(jnp.int32, (1, total), 1)
    token = (index % block // rows * n_tensor + index // block) * rows + index % rows
    usable = token < live
    factor = HS ** (-0.5) * math.log2(math.e)

    def slot_of(side):
        return (side + s) % 2

    def att_copy(h, step, target, source, side=None):
        first, count, slot = (0, block, 0) if side is None else (side * rows, rows, slot_of(side))
        here = pl.ds(pl.multiple_of(target * block + first, rows), count)
        there = pl.ds(pl.multiple_of(first, rows), count)
        cols = pl.ds(pl.multiple_of((source * heads + h) * HS, HS), HS)
        return remote(
            done.at[h, here, :], mixed.at[there, cols],
            att_send.at[h, slot, step], att_recv.at[h, slot, step], device(s, target, b),
        )

    def attend(h, target, first, count):
        here = pl.ds(pl.multiple_of(target * block + first, rows), count)
        scores = lax.dot_general(
            got[h, 0, here, :], got[h, 1], (((1,), (1,)), ((), ())), preferred_element_type=jnp.float32
        )
        scores = jnp.where(usable, scores, MASKED_SCORE)
        peak = jnp.max(scores, axis=-1, keepdims=True)
        expo = jnp.exp2((scores - peak) * factor)
        denominator = jnp.sum(expo, axis=-1, keepdims=True)
        result = jnp.dot(expo.astype(jnp.bfloat16), got[h, 2], preferred_element_type=jnp.float32) / denominator
        row = first + lax.broadcasted_iota(jnp.int32, (count, 1), 0)
        own_token = (row // rows * n_tensor + target) * rows + row % rows
        return jnp.where(own_token < live, result, 0.0).astype(jnp.bfloat16)

    def attend_all(h, first, count, side):
        def one(step, carry):
            target = (t + step) % n_tensor
            done[h, pl.ds(pl.multiple_of(target * block + first, rows), count), :] = attend(h, target, first, count)
            att_copy(h, step, target, t, side).start()
            return carry

        lax.fori_loop(1, n_tensor, one, 0)
        mixed[
            pl.ds(pl.multiple_of(first, rows), count), pl.ds(pl.multiple_of((t * heads + h) * HS, HS), HS)
        ] = attend(h, t, first, count)

    relayed = 1
    for h in range(heads):
        if relayed < n_tensor:
            relay(relayed)
            relayed += 1
        if h + 1 < heads:
            start_qkv(h + 1)

        def arrive(step, carry):
            source = (me + group - step) % group
            for j in range(3):
                qkv_copy(h, j, step, me, source).wait_recv()
            return carry

        lax.fori_loop(1, group, arrive, 0)
        if h + 1 < heads:
            attend_all(h, 0, block, None)
        else:
            attend_all(h, (1 - s) * rows, rows, 1 - s)
            attend_all(h, s * rows, rows, s)
    for k in range(relayed, n_tensor):
        relay(k)

    for p in range(n_tensor):
        far_copy(p, far).wait_recv()
        near_copy(1, p, far).start()
    for p in range(n_tensor):
        near_copy(0, p, near).wait_recv()
        near_copy(1, p, (near + 2) % 4).wait_recv()
    def back(h, side):
        def body(step, carry):
            att_copy(h, step, t, (t + n_tensor - step) % n_tensor, side).wait_recv()
            return carry

        lax.fori_loop(1, n_tensor, body, 0)

    def part_copy(p):
        cut = slice(p * w_cols, (p + 1) * w_cols)
        return remote(
            part_out.at[:, cut], part_in.at[:, cut], part_send.at[p], part_recv.at[p], device(1 - s, t, b)
        )

    def leave(p):
        cut = slice(p * w_cols, (p + 1) * w_cols)
        return pltpu.make_async_copy(part_in.at[:, cut], out_ref.at[0, :, cut], out_sem.at[p])

    for h in range(heads - 1):
        back(h, None)
    back(heads - 1, 1 - s)
    for p in range(n_tensor):
        cut = slice(p * w_cols, (p + 1) * w_cols)
        part_out[:, cut] = jnp.dot(
            mixed[pl.ds(pl.multiple_of((1 - s) * rows, rows), rows), :], weight[:, cut],
            preferred_element_type=jnp.float32,
        ).astype(jnp.bfloat16)
        part_copy(p).start()
    back(heads - 1, s)
    for p in range(n_tensor):
        cut = slice(p * w_cols, (p + 1) * w_cols)
        own_part[:, cut] = jnp.dot(
            mixed[pl.ds(pl.multiple_of(s * rows, rows), rows), :], weight[:, cut],
            preferred_element_type=jnp.float32,
        )
    for p in range(n_tensor):
        cut = slice(p * w_cols, (p + 1) * w_cols)
        part_copy(p).wait_recv()
        part_in[:, cut] = (own_part[:, cut] + part_in[:, cut].astype(jnp.float32)).astype(jnp.bfloat16)
        leave(p).start()

    for h in range(heads):
        def sent(step, carry):
            peer = (me + step) % group
            for j in range(3):
                qkv_copy(h, j, step, peer, me).wait_send()
            return carry

        lax.fori_loop(1, group, sent, 0)

        def att_sent(step, carry):
            if h + 1 < heads:
                att_copy(h, step, (t + step) % n_tensor, t).wait_send()
            else:
                att_copy(h, step, (t + step) % n_tensor, t, 1 - s).wait_send()
                att_copy(h, step, (t + step) % n_tensor, t, s).wait_send()
            return carry

        lax.fori_loop(1, n_tensor, att_sent, 0)
    for k in range(n_tensor):
        @pl.when((t >= k) & (t < n_tensor - 1))
        def _():
            up_copy(t - k).wait_send()

        @pl.when((t + k < n_tensor) & (t > 0))
        def _():
            down_copy(t + k).wait_send()

    for p in range(n_tensor):
        far_copy(p, b).wait_send()
        near_copy(0, p, b).wait_send()
        near_copy(1, p, far).wait_send()
        part_copy(p).wait_send()
        leave(p).wait()


def fused(axes, sizes, queries, keys, values, lengths, out_weight):
    n_seq, n_tensor, n_bucket = sizes
    rows, width = queries.shape[1:]
    group = n_seq * n_tensor
    heads = width // HS // group
    total = group * rows
    half = width // n_seq
    vmem = pl.BlockSpec(memory_space=pltpu.VMEM)
    dma = pltpu.SemaphoreType.DMA
    return pl.pallas_call(
        functools.partial(whole_kernel, axes, sizes),
        out_shape=jax.ShapeDtypeStruct(queries.shape, queries.dtype),
        in_specs=[pl.BlockSpec(memory_space=pltpu.SMEM), vmem, vmem, vmem, vmem],
        out_specs=pl.BlockSpec(memory_space=pl.ANY),
        scratch_shapes=[
            pltpu.VMEM((heads, 3, total, HS), jnp.bfloat16),
            pltpu.VMEM((heads, total, HS), jnp.bfloat16),
            pltpu.VMEM((n_seq * rows, half), jnp.bfloat16),
            pltpu.VMEM((half, width), jnp.bfloat16),
            pltpu.VMEM((rows, width), jnp.bfloat16),
            pltpu.VMEM((rows, width), jnp.bfloat16),
            pltpu.VMEM((rows, width), jnp.float32),
            dma((heads, 3, group)),
            dma((heads, 3, group)),
            dma((heads, 2, n_tensor)),
            dma((heads, 2, n_tensor)),
            dma((n_tensor,)),
            dma((n_tensor,)),
            dma((n_tensor,)),
            dma((n_tensor,)),
            dma((n_tensor,)),
            dma((2, n_tensor)),
            dma((2, n_tensor)),
            dma((n_tensor,)),
            dma((n_tensor,)),
            dma((n_tensor,)),
        ],
        compiler_params=pltpu.CompilerParams(has_side_effects=True, vmem_limit_bytes=56 * 1024 * 1024),
    )(lengths, queries, keys, values, out_weight)


def solution(mesh):
    in_specs = (
        P("bucket", ("seq", "tensor"), None),
        P("bucket", ("seq", "tensor"), None),
        P("bucket", ("seq", "tensor"), None),
        P("bucket"),
        P(("seq", "bucket"), "tensor"),
    )
    out_specs = P("bucket", ("seq", "tensor"), None)
    sizes = tuple(mesh.shape[name] for name in ("seq", "tensor", "bucket"))

    def step(queries, keys, values, lengths, out_weight):
        head_count = queries.shape[2] // HS
        fits = sizes[0] == 2 and sizes[1] == sizes[2] == 4 and head_count % (sizes[0] * sizes[1]) == 0
        if fits:
            return fused(mesh.axis_names, sizes, queries, keys, values, lengths, out_weight)
        return shards(queries, keys, values, lengths, out_weight)

    return jax.shard_map(step, mesh=mesh, in_specs=in_specs, out_specs=out_specs, check_vma=False)
```

```python
import functools
import math

import jax
import jax.numpy as jnp
from jax import lax
from jax.experimental import pallas as pl
from jax.experimental.pallas import tpu as pltpu
from jax.sharding import PartitionSpec as P

HS = 128


MASKED_SCORE = -1e30


def shards(queries, keys, values, lengths, out_weight):
    tok_rows = queries.shape[1]
    n_tensor = lax.axis_size("tensor")
    tensor_index = lax.axis_index("tensor")
    live_len = lengths[0]
    local_q, local_k, local_v = (
        lax.all_to_all(queries[0], "seq", split_axis=1, concat_axis=0, tiled=True),
        lax.all_to_all(keys[0], "seq", split_axis=1, concat_axis=0, tiled=True),
        lax.all_to_all(values[0], "seq", split_axis=1, concat_axis=0, tiled=True),
    )
    row_count, col_count = local_q.shape
    head_count = col_count // HS
    query_heads = local_q.reshape(row_count, head_count, HS)

    def spots(first_row, total_rows):
        index_row = first_row + jnp.arange(total_rows, dtype=jnp.int32)
        owner = index_row // row_count
        within = index_row % row_count
        return (within // tok_rows * n_tensor + owner) * tok_rows + within % tok_rows

    query_usable = spots(tensor_index * row_count, row_count) < live_len
    initial = (
        jnp.full((row_count, head_count), MASKED_SCORE, jnp.float32),
        jnp.zeros((row_count, head_count), jnp.float32),
        jnp.zeros((row_count, head_count, HS), jnp.float32),
    )
    carried = initial
    first_row = jnp.int32(0)
    key_rows = lax.all_gather(local_k, "tensor", axis=0, tiled=True)
    value_rows = lax.all_gather(local_v, "tensor", axis=0, tiled=True)
    for offset in range(key_rows.shape[0] // row_count):
        row_peak, row_sum, accumulated = carried
        key_tile = key_rows[offset * row_count : (offset + 1) * row_count].reshape(
            row_count, head_count, HS
        )
        value_tile = value_rows[offset * row_count : (offset + 1) * row_count].reshape(
            row_count, head_count, HS
        )
        key_usable = spots(first_row + offset * row_count, row_count) < live_len
        scores = jnp.einsum(
            "qhd,khd->qhk", query_heads, key_tile, preferred_element_type=jnp.float32
        ) * HS ** (-0.5)
        scores = jnp.where(key_usable[None, None, :], scores, MASKED_SCORE)
        peak_new = jnp.maximum(row_peak, jnp.max(scores, axis=-1))
        exponent = jnp.where(key_usable[None, None, :], jnp.exp(scores - peak_new[..., None]), 0.0)
        rescale = jnp.exp(row_peak - peak_new)
        accumulated = accumulated * rescale[..., None] + jnp.einsum(
            "qhk,khd->qhd",
            exponent.astype(jnp.bfloat16),
            value_tile,
            preferred_element_type=jnp.float32,
        )
        carried = (peak_new, row_sum * rescale + jnp.sum(exponent, axis=-1), accumulated)
    row_peak, row_sum, accumulated = carried
    attended = accumulated / row_sum[..., None]
    mixed = jnp.where(query_usable[:, None], attended.reshape(row_count, col_count), 0.0).astype(
        jnp.bfloat16
    )
    restored = lax.all_to_all(mixed, "seq", split_axis=0, concat_axis=1, tiled=True)
    wide_weight = lax.all_gather(out_weight, "tensor", axis=1, tiled=True)
    summed = jnp.dot(
        restored,
        lax.all_gather(wide_weight, ("seq", "bucket"), axis=0, tiled=True),
        preferred_element_type=jnp.float32,
    )
    return summed.astype(jnp.bfloat16)[None]


def whole_kernel(
    axes, sizes, len_ref, q_ref, k_ref, v_ref, w_ref, out_ref,
    got, done, mixed, weight, part_out, part_in, own_part,
    qkv_send, qkv_recv, att_send, att_recv, up_send, down_send, line_recv,
    far_send, far_recv, near_send, near_recv, part_send, part_recv, out_sem,
):
    n_seq, n_tensor, n_bucket = sizes
    s, t, b = lax.axis_index("seq"), lax.axis_index("tensor"), lax.axis_index("bucket")
    group = n_seq * n_tensor
    rows = q_ref.shape[1]
    width = q_ref.shape[2]
    heads = width // HS // group
    w_rows, w_cols = w_ref.shape
    block = n_seq * rows
    live = len_ref[0]

    def device(ds, dt, db):
        place = {"seq": ds, "tensor": dt, "bucket": db}
        return tuple(place[name] for name in axes)

    def remote(src, dst, send, recv, where):
        return pltpu.make_async_remote_copy(
            src_ref=src, dst_ref=dst, send_sem=send, recv_sem=recv,
            device_id=where, device_id_type=pl.DeviceIdType.MESH,
        )

    me = s * n_tensor + t
    streams = (q_ref, k_ref, v_ref)

    def spot(ds, dt):
        return pl.ds(pl.multiple_of((dt * n_seq + ds) * rows, rows), rows)

    def qkv_copy(h, j, step, peer, source):
        cols = pl.ds(pl.multiple_of((peer * heads + h) * HS, HS), HS)
        return remote(
            streams[j].at[0, :, cols],
            got.at[h, j, spot(source // n_tensor, source % n_tensor), :],
            qkv_send.at[h, j, step],
            qkv_recv.at[h, j, step],
            device(peer // n_tensor, peer % n_tensor, b),
        )

    def start_qkv(h):
        def body(step, carry):
            peer = (me + step) % group
            for j in range(3):
                qkv_copy(h, j, step, peer, me).start()
            return carry

        lax.fori_loop(1, group, body, 0)

    def piece(row_block, col_block):
        return weight.at[
            pl.ds(pl.multiple_of(row_block * w_rows, w_rows), w_rows),
            pl.ds(pl.multiple_of(col_block * w_cols, w_cols), w_cols),
        ]

    far, near = (b + 2) % 4, b + 1 - 2 * (b % 2)

    def up_copy(p):
        return remote(piece(b, p), piece(b, p), up_send.at[p], line_recv.at[p], device(s, t + 1, b))

    def down_copy(p):
        return remote(piece(b, p), piece(b, p), down_send.at[p], line_recv.at[p], device(s, t - 1, b))

    def far_copy(p, row_block):
        return remote(piece(row_block, p), piece(row_block, p), far_send.at[p], far_recv.at[p], device(s, t, far))

    def near_copy(k, p, row_block):
        return remote(
            piece(row_block, p), piece(row_block, p), near_send.at[k, p], near_recv.at[k, p], device(s, t, near)
        )

    def spread(p):
        far_copy(p, b).start()
        near_copy(0, p, b).start()

    def relay(k):
        @pl.when(t >= k)
        def _():
            up_copy(t - k).wait_recv()

            @pl.when(t < n_tensor - 1)
            def _():
                up_copy(t - k).start()

            spread(t - k)

        @pl.when(t + k < n_tensor)
        def _():
            down_copy(t + k).wait_recv()

            @pl.when(t > 0)
            def _():
                down_copy(t + k).start()

            spread(t + k)

    weight[
        pl.ds(pl.multiple_of(b * w_rows, w_rows), w_rows),
        pl.ds(pl.multiple_of(t * w_cols, w_cols), w_cols),
    ] = w_ref[...]

    @pl.when(t < n_tensor - 1)
    def _():
        up_copy(t).start()

    @pl.when(t > 0)
    def _():
        down_copy(t).start()

    start_qkv(0)
    spread(t)

    for h in range(heads):
        cols = pl.ds(pl.multiple_of((me * heads + h) * HS, HS), HS)
        for j in range(3):
            got[h, j, spot(s, t), :] = streams[j][0, :, cols]

    total = group * rows
    index = lax.broadcasted_iota(jnp.int32, (1, total), 1)
    token = (index % block // rows * n_tensor + index // block) * rows + index % rows
    usable = token < live
    factor = HS ** (-0.5) * math.log2(math.e)

    def slot_of(side):
        return (side + s) % 2

    def att_copy(h, step, target, source, side=None):
        first, count, slot = (0, block, 0) if side is None else (side * rows, rows, slot_of(side))
        here = pl.ds(pl.multiple_of(target * block + first, rows), count)
        there = pl.ds(pl.multiple_of(first, rows), count)
        cols = pl.ds(pl.multiple_of((source * heads + h) * HS, HS), HS)
        return remote(
            done.at[h, here, :], mixed.at[there, cols],
            att_send.at[h, slot, step], att_recv.at[h, slot, step], device(s, target, b),
        )

    def attend(h, target, first, count):
        here = pl.ds(pl.multiple_of(target * block + first, rows), count)
        scores = lax.dot_general(
            got[h, 0, here, :], got[h, 1], (((1,), (1,)), ((), ())), preferred_element_type=jnp.float32
        )
        scores = jnp.where(usable, scores, MASKED_SCORE)
        peak = jnp.max(scores, axis=-1, keepdims=True)
        expo = jnp.exp2((scores - peak) * factor)
        denominator = jnp.sum(expo, axis=-1, keepdims=True)
        result = jnp.dot(expo.astype(jnp.bfloat16), got[h, 2], preferred_element_type=jnp.float32) / denominator
        row = first + lax.broadcasted_iota(jnp.int32, (count, 1), 0)
        own_token = (row // rows * n_tensor + target) * rows + row % rows
        return jnp.where(own_token < live, result, 0.0).astype(jnp.bfloat16)

    def attend_all(h, first, count, side):
        def one(step, carry):
            target = (t + step) % n_tensor
            done[h, pl.ds(pl.multiple_of(target * block + first, rows), count), :] = attend(h, target, first, count)
            att_copy(h, step, target, t, side).start()
            return carry

        lax.fori_loop(1, n_tensor, one, 0)
        mixed[
            pl.ds(pl.multiple_of(first, rows), count), pl.ds(pl.multiple_of((t * heads + h) * HS, HS), HS)
        ] = attend(h, t, first, count)

    upper = t // 2
    order = (t, 1 - t + 4 * upper, 2 - upper, 3 - 3 * upper)

    def forward(p):
        far_copy(p, far).wait_recv()
        near_copy(1, p, far).start()

    for h in range(heads):
        if h == 0:
            relay(1)
            for later in range(1, heads):
                start_qkv(later)
        elif h == 1:
            relay(2)

        def arrive(step, carry):
            source = (me + group - step) % group
            for j in range(3):
                qkv_copy(h, j, step, me, source).wait_recv()
            return carry

        lax.fori_loop(1, group, arrive, 0)
        if 1 <= h <= 2:
            forward(order[h - 1])
        if h + 1 < heads:
            attend_all(h, 0, block, None)
        else:
            attend_all(h, (1 - s) * rows, rows, 1 - s)
            attend_all(h, s * rows, rows, s)
    for k in range(heads, 3):
        relay(k)
    for k in range(max(heads - 1, 0), 3):
        forward(order[k])

    def back(h, side):
        def body(step, carry):
            att_copy(h, step, t, (t + n_tensor - step) % n_tensor, side).wait_recv()
            return carry

        lax.fori_loop(1, n_tensor, body, 0)

    def cut_of(p):
        return pl.ds(pl.multiple_of(p * w_cols, w_cols), w_cols)

    def part_copy(p):
        cut = cut_of(p)
        return remote(
            part_out.at[:, cut], part_in.at[:, cut], part_send.at[p], part_recv.at[p], device(1 - s, t, b)
        )

    def leave(p):
        cut = cut_of(p)
        return pltpu.make_async_copy(part_in.at[:, cut], out_ref.at[0, :, cut], out_sem.at[p])

    for h in range(heads - 1):
        back(h, None)
    back(heads - 1, 1 - s)
    for k, p in enumerate(order):
        near_copy(0, p, near).wait_recv()
        near_copy(1, p, (near + 2) % 4).wait_recv()
        cut = cut_of(p)
        part_out[:, cut] = jnp.dot(
            mixed[pl.ds(pl.multiple_of((1 - s) * rows, rows), rows), :], weight[:, cut],
            preferred_element_type=jnp.float32,
        ).astype(jnp.bfloat16)
        part_copy(p).start()
        if k == 0:
            relay(3)
        if k == 2:
            forward(order[3])
    back(heads - 1, s)
    for p in order:
        cut = cut_of(p)
        own_part[:, cut] = jnp.dot(
            mixed[pl.ds(pl.multiple_of(s * rows, rows), rows), :], weight[:, cut],
            preferred_element_type=jnp.float32,
        )
    for p in order:
        cut = cut_of(p)
        part_copy(p).wait_recv()
        part_in[:, cut] = (own_part[:, cut] + part_in[:, cut].astype(jnp.float32)).astype(jnp.bfloat16)
        leave(p).start()

    for h in range(heads):
        def sent(step, carry):
            peer = (me + step) % group
            for j in range(3):
                qkv_copy(h, j, step, peer, me).wait_send()
            return carry

        lax.fori_loop(1, group, sent, 0)

        def att_sent(step, carry):
            if h + 1 < heads:
                att_copy(h, step, (t + step) % n_tensor, t).wait_send()
            else:
                att_copy(h, step, (t + step) % n_tensor, t, 1 - s).wait_send()
                att_copy(h, step, (t + step) % n_tensor, t, s).wait_send()
            return carry

        lax.fori_loop(1, n_tensor, att_sent, 0)
    for k in range(n_tensor):
        @pl.when((t >= k) & (t < n_tensor - 1))
        def _():
            up_copy(t - k).wait_send()

        @pl.when((t + k < n_tensor) & (t > 0))
        def _():
            down_copy(t + k).wait_send()

    for p in range(n_tensor):
        far_copy(p, b).wait_send()
        near_copy(0, p, b).wait_send()
        near_copy(1, p, far).wait_send()
        part_copy(p).wait_send()
        leave(p).wait()


def fused(axes, sizes, queries, keys, values, lengths, out_weight):
    n_seq, n_tensor, n_bucket = sizes
    rows, width = queries.shape[1:]
    group = n_seq * n_tensor
    heads = width // HS // group
    total = group * rows
    half = width // n_seq
    vmem = pl.BlockSpec(memory_space=pltpu.VMEM)
    dma = pltpu.SemaphoreType.DMA
    return pl.pallas_call(
        functools.partial(whole_kernel, axes, sizes),
        out_shape=jax.ShapeDtypeStruct(queries.shape, queries.dtype),
        in_specs=[pl.BlockSpec(memory_space=pltpu.SMEM), vmem, vmem, vmem, vmem],
        out_specs=pl.BlockSpec(memory_space=pl.ANY),
        scratch_shapes=[
            pltpu.VMEM((heads, 3, total, HS), jnp.bfloat16),
            pltpu.VMEM((heads, total, HS), jnp.bfloat16),
            pltpu.VMEM((n_seq * rows, half), jnp.bfloat16),
            pltpu.VMEM((half, width), jnp.bfloat16),
            pltpu.VMEM((rows, width), jnp.bfloat16),
            pltpu.VMEM((rows, width), jnp.bfloat16),
            pltpu.VMEM((rows, width), jnp.float32),
            dma((heads, 3, group)),
            dma((heads, 3, group)),
            dma((heads, 2, n_tensor)),
            dma((heads, 2, n_tensor)),
            dma((n_tensor,)),
            dma((n_tensor,)),
            dma((n_tensor,)),
            dma((n_tensor,)),
            dma((n_tensor,)),
            dma((2, n_tensor)),
            dma((2, n_tensor)),
            dma((n_tensor,)),
            dma((n_tensor,)),
            dma((n_tensor,)),
        ],
        compiler_params=pltpu.CompilerParams(has_side_effects=True, vmem_limit_bytes=56 * 1024 * 1024),
    )(lengths, queries, keys, values, out_weight)


def solution(mesh):
    in_specs = (
        P("bucket", ("seq", "tensor"), None),
        P("bucket", ("seq", "tensor"), None),
        P("bucket", ("seq", "tensor"), None),
        P("bucket"),
        P(("seq", "bucket"), "tensor"),
    )
    out_specs = P("bucket", ("seq", "tensor"), None)
    sizes = tuple(mesh.shape[name] for name in ("seq", "tensor", "bucket"))

    def step(queries, keys, values, lengths, out_weight):
        head_count = queries.shape[2] // HS
        fits = sizes[0] == 2 and sizes[1] == sizes[2] == 4 and head_count % (sizes[0] * sizes[1]) == 0
        if fits:
            return fused(mesh.axis_names, sizes, queries, keys, values, lengths, out_weight)
        return shards(queries, keys, values, lengths, out_weight)

    return jax.shard_map(step, mesh=mesh, in_specs=in_specs, out_specs=out_specs, check_vma=False)
```

```python
import functools
import math

import jax
import jax.numpy as jnp
from jax import lax
from jax.experimental import pallas as pl
from jax.experimental.pallas import tpu as pltpu
from jax.sharding import PartitionSpec as P

HS = 128


MASKED_SCORE = -1e30


def shards(queries, keys, values, lengths, out_weight):
    tok_rows = queries.shape[1]
    n_tensor = lax.axis_size("tensor")
    tensor_index = lax.axis_index("tensor")
    live_len = lengths[0]
    local_q, local_k, local_v = (
        lax.all_to_all(queries[0], "seq", split_axis=1, concat_axis=0, tiled=True),
        lax.all_to_all(keys[0], "seq", split_axis=1, concat_axis=0, tiled=True),
        lax.all_to_all(values[0], "seq", split_axis=1, concat_axis=0, tiled=True),
    )
    row_count, col_count = local_q.shape
    head_count = col_count // HS
    query_heads = local_q.reshape(row_count, head_count, HS)

    def spots(first_row, total_rows):
        index_row = first_row + jnp.arange(total_rows, dtype=jnp.int32)
        owner = index_row // row_count
        within = index_row % row_count
        return (within // tok_rows * n_tensor + owner) * tok_rows + within % tok_rows

    query_usable = spots(tensor_index * row_count, row_count) < live_len
    initial = (
        jnp.full((row_count, head_count), MASKED_SCORE, jnp.float32),
        jnp.zeros((row_count, head_count), jnp.float32),
        jnp.zeros((row_count, head_count, HS), jnp.float32),
    )
    carried = initial
    first_row = jnp.int32(0)
    key_rows = lax.all_gather(local_k, "tensor", axis=0, tiled=True)
    value_rows = lax.all_gather(local_v, "tensor", axis=0, tiled=True)
    for offset in range(key_rows.shape[0] // row_count):
        row_peak, row_sum, accumulated = carried
        key_tile = key_rows[offset * row_count : (offset + 1) * row_count].reshape(
            row_count, head_count, HS
        )
        value_tile = value_rows[offset * row_count : (offset + 1) * row_count].reshape(
            row_count, head_count, HS
        )
        key_usable = spots(first_row + offset * row_count, row_count) < live_len
        scores = jnp.einsum(
            "qhd,khd->qhk", query_heads, key_tile, preferred_element_type=jnp.float32
        ) * HS ** (-0.5)
        scores = jnp.where(key_usable[None, None, :], scores, MASKED_SCORE)
        peak_new = jnp.maximum(row_peak, jnp.max(scores, axis=-1))
        exponent = jnp.where(key_usable[None, None, :], jnp.exp(scores - peak_new[..., None]), 0.0)
        rescale = jnp.exp(row_peak - peak_new)
        accumulated = accumulated * rescale[..., None] + jnp.einsum(
            "qhk,khd->qhd",
            exponent.astype(jnp.bfloat16),
            value_tile,
            preferred_element_type=jnp.float32,
        )
        carried = (peak_new, row_sum * rescale + jnp.sum(exponent, axis=-1), accumulated)
    row_peak, row_sum, accumulated = carried
    attended = accumulated / row_sum[..., None]
    mixed = jnp.where(query_usable[:, None], attended.reshape(row_count, col_count), 0.0).astype(
        jnp.bfloat16
    )
    restored = lax.all_to_all(mixed, "seq", split_axis=0, concat_axis=1, tiled=True)
    wide_weight = lax.all_gather(out_weight, "tensor", axis=1, tiled=True)
    summed = jnp.dot(
        restored,
        lax.all_gather(wide_weight, ("seq", "bucket"), axis=0, tiled=True),
        preferred_element_type=jnp.float32,
    )
    return summed.astype(jnp.bfloat16)[None]


def whole_kernel(
    axes, sizes, len_ref, q_ref, k_ref, v_ref, w_ref, out_ref,
    got, done, mixed, weight, part_out, part_in, own_part,
    qkv_send, qkv_recv, att_send, att_recv, up_send, down_send, line_recv,
    far_send, far_recv, near_send, near_recv, part_send, part_recv, out_sem,
):
    n_seq, n_tensor, n_bucket = sizes
    s, t, b = lax.axis_index("seq"), lax.axis_index("tensor"), lax.axis_index("bucket")
    group = n_seq * n_tensor
    rows = q_ref.shape[1]
    width = q_ref.shape[2]
    heads = width // HS // group
    w_rows, w_cols = w_ref.shape
    block = n_seq * rows
    live = len_ref[0]

    def device(ds, dt, db):
        place = {"seq": ds, "tensor": dt, "bucket": db}
        return tuple(place[name] for name in axes)

    def remote(src, dst, send, recv, where):
        return pltpu.make_async_remote_copy(
            src_ref=src, dst_ref=dst, send_sem=send, recv_sem=recv,
            device_id=where, device_id_type=pl.DeviceIdType.MESH,
        )

    me = s * n_tensor + t
    streams = (q_ref, k_ref, v_ref)

    def spot(ds, dt):
        return pl.ds(pl.multiple_of((dt * n_seq + ds) * rows, rows), rows)

    def qkv_copy(h, j, step, peer, source):
        cols = pl.ds(pl.multiple_of((peer * heads + h) * HS, HS), HS)
        return remote(
            streams[j].at[0, :, cols],
            got.at[h, j, spot(source // n_tensor, source % n_tensor), :],
            qkv_send.at[h, j, step],
            qkv_recv.at[h, j, step],
            device(peer // n_tensor, peer % n_tensor, b),
        )

    def start_qkv(h):
        def body(step, carry):
            peer = (me + step) % group
            for j in range(3):
                qkv_copy(h, j, step, peer, me).start()
            return carry

        lax.fori_loop(1, group, body, 0)

    def piece(row_block, col_block):
        return weight.at[
            pl.ds(pl.multiple_of(row_block * w_rows, w_rows), w_rows),
            pl.ds(pl.multiple_of(col_block * w_cols, w_cols), w_cols),
        ]

    far, near = (b + 2) % 4, b + 1 - 2 * (b % 2)

    def up_copy(p):
        return remote(piece(b, p), piece(b, p), up_send.at[p], line_recv.at[p], device(s, t + 1, b))

    def down_copy(p):
        return remote(piece(b, p), piece(b, p), down_send.at[p], line_recv.at[p], device(s, t - 1, b))

    def far_copy(p, row_block):
        return remote(piece(row_block, p), piece(row_block, p), far_send.at[p], far_recv.at[p], device(s, t, far))

    def near_copy(k, p, row_block):
        return remote(
            piece(row_block, p), piece(row_block, p), near_send.at[k, p], near_recv.at[k, p], device(s, t, near)
        )

    def spread(p):
        far_copy(p, b).start()
        near_copy(0, p, b).start()

    def relay(k):
        @pl.when(t >= k)
        def _():
            up_copy(t - k).wait_recv()

            @pl.when(t < n_tensor - 1)
            def _():
                up_copy(t - k).start()

            spread(t - k)

        @pl.when(t + k < n_tensor)
        def _():
            down_copy(t + k).wait_recv()

            @pl.when(t > 0)
            def _():
                down_copy(t + k).start()

            spread(t + k)

    weight[
        pl.ds(pl.multiple_of(b * w_rows, w_rows), w_rows),
        pl.ds(pl.multiple_of(t * w_cols, w_cols), w_cols),
    ] = w_ref[...]

    @pl.when(t < n_tensor - 1)
    def _():
        up_copy(t).start()

    @pl.when(t > 0)
    def _():
        down_copy(t).start()

    start_qkv(0)
    spread(t)

    for h in range(heads):
        cols = pl.ds(pl.multiple_of((me * heads + h) * HS, HS), HS)
        for j in range(3):
            got[h, j, spot(s, t), :] = streams[j][0, :, cols]

    total = group * rows
    index = lax.broadcasted_iota(jnp.int32, (1, total), 1)
    token = (index % block // rows * n_tensor + index // block) * rows + index % rows
    usable = token < live
    factor = HS ** (-0.5) * math.log2(math.e)

    def slot_of(side):
        return (side + s) % 2

    def att_copy(h, step, target, source, side=None):
        first, count, slot = (0, block, 0) if side is None else (side * rows, rows, slot_of(side))
        here = pl.ds(pl.multiple_of(target * block + first, rows), count)
        there = pl.ds(pl.multiple_of(first, rows), count)
        cols = pl.ds(pl.multiple_of((source * heads + h) * HS, HS), HS)
        return remote(
            done.at[h, here, :], mixed.at[there, cols],
            att_send.at[h, slot, step], att_recv.at[h, slot, step], device(s, target, b),
        )

    def attend(h, target, first, count):
        here = pl.ds(pl.multiple_of(target * block + first, rows), count)
        row = first + lax.broadcasted_iota(jnp.int32, (count, 1), 0)
        return attend_rows(h, got[h, 0, here, :], (row // rows * n_tensor + target) * rows + row % rows)

    def attend_rows(h, query, own_token):
        scores = lax.dot_general(
            query, got[h, 1], (((1,), (1,)), ((), ())), preferred_element_type=jnp.float32
        )
        scores = jnp.where(usable, scores, MASKED_SCORE)
        peak = jnp.max(scores, axis=-1, keepdims=True)
        expo = jnp.exp2((scores - peak) * factor)
        denominator = jnp.sum(expo, axis=-1, keepdims=True)
        result = jnp.dot(expo.astype(jnp.bfloat16), got[h, 2], preferred_element_type=jnp.float32) / denominator
        return jnp.where(own_token < live, result, 0.0).astype(jnp.bfloat16)

    def attend_all(h, first, count, side):
        def one(step, carry):
            target = (t + step) % n_tensor
            done[h, pl.ds(pl.multiple_of(target * block + first, rows), count), :] = attend(h, target, first, count)
            att_copy(h, step, target, t, side).start()
            return carry

        lax.fori_loop(1, n_tensor, one, 0)
        mixed[
            pl.ds(pl.multiple_of(first, rows), count), pl.ds(pl.multiple_of((t * heads + h) * HS, HS), HS)
        ] = attend(h, t, first, count)

    def attend_side(h, side):
        row = lax.broadcasted_iota(jnp.int32, (rows, 1), 0)
        for step in range(0, n_tensor, 2):
            targets = [(t + step + i) % n_tensor for i in (1, 2)]
            spans = [pl.ds(pl.multiple_of(target * block + side * rows, rows), rows) for target in targets]
            result = attend_rows(
                h,
                jnp.concatenate([got[h, 0, span, :] for span in spans], axis=0),
                jnp.concatenate([(side * n_tensor + target) * rows + row for target in targets], axis=0),
            )
            for i in range(2):
                if step + i + 1 < n_tensor:
                    done[h, spans[i], :] = result[i * rows : (i + 1) * rows]
                    att_copy(h, step + i + 1, targets[i], t, side).start()
                else:
                    mixed[
                        pl.ds(pl.multiple_of(side * rows, rows), rows),
                        pl.ds(pl.multiple_of((t * heads + h) * HS, HS), HS),
                    ] = result[i * rows : (i + 1) * rows]

    upper = t // 2
    order = (t, 1 - t + 4 * upper, 2 - upper, 3 - 3 * upper)

    def forward(p):
        far_copy(p, far).wait_recv()
        near_copy(1, p, far).start()

    for h in range(heads):
        if h == 0:
            relay(1)
            for later in range(1, heads):
                start_qkv(later)
        elif h == 1:
            relay(2)

        def arrive(step, carry):
            source = (me + group - step) % group
            for j in range(3):
                qkv_copy(h, j, step, me, source).wait_recv()
            return carry

        lax.fori_loop(1, group, arrive, 0)
        if 1 <= h <= 2:
            forward(order[h - 1])
        if h + 1 < heads:
            attend_all(h, 0, block, None)
        else:
            attend_side(h, 1 - s)
            attend_side(h, s)
    for k in range(heads, 3):
        relay(k)
    for k in range(max(heads - 1, 0), 3):
        forward(order[k])

    def back(h, side):
        def body(step, carry):
            att_copy(h, step, t, (t + n_tensor - step) % n_tensor, side).wait_recv()
            return carry

        lax.fori_loop(1, n_tensor, body, 0)

    def cut_of(p):
        return pl.ds(pl.multiple_of(p * w_cols, w_cols), w_cols)

    def part_copy(p):
        cut = cut_of(p)
        return remote(
            part_out.at[:, cut], part_in.at[:, cut], part_send.at[p], part_recv.at[p], device(1 - s, t, b)
        )

    def leave(p):
        cut = cut_of(p)
        return pltpu.make_async_copy(part_in.at[:, cut], out_ref.at[0, :, cut], out_sem.at[p])

    for h in range(heads - 1):
        back(h, None)
    back(heads - 1, 1 - s)
    for k, p in enumerate(order):
        near_copy(0, p, near).wait_recv()
        near_copy(1, p, (near + 2) % 4).wait_recv()
        cut = cut_of(p)
        part_out[:, cut] = jnp.dot(
            mixed[pl.ds(pl.multiple_of((1 - s) * rows, rows), rows), :], weight[:, cut],
            preferred_element_type=jnp.float32,
        ).astype(jnp.bfloat16)
        part_copy(p).start()
        if k == 0:
            relay(3)
        if k == 2:
            forward(order[3])
    back(heads - 1, s)
    for p in order:
        cut = cut_of(p)
        own_part[:, cut] = jnp.dot(
            mixed[pl.ds(pl.multiple_of(s * rows, rows), rows), :], weight[:, cut],
            preferred_element_type=jnp.float32,
        )
    for p in order:
        cut = cut_of(p)
        part_copy(p).wait_recv()
        part_in[:, cut] = (own_part[:, cut] + part_in[:, cut].astype(jnp.float32)).astype(jnp.bfloat16)
        leave(p).start()

    for h in range(heads):
        def sent(step, carry):
            peer = (me + step) % group
            for j in range(3):
                qkv_copy(h, j, step, peer, me).wait_send()
            return carry

        lax.fori_loop(1, group, sent, 0)

        def att_sent(step, carry):
            if h + 1 < heads:
                att_copy(h, step, (t + step) % n_tensor, t).wait_send()
            else:
                att_copy(h, step, (t + step) % n_tensor, t, 1 - s).wait_send()
                att_copy(h, step, (t + step) % n_tensor, t, s).wait_send()
            return carry

        lax.fori_loop(1, n_tensor, att_sent, 0)
    for k in range(n_tensor):
        @pl.when((t >= k) & (t < n_tensor - 1))
        def _():
            up_copy(t - k).wait_send()

        @pl.when((t + k < n_tensor) & (t > 0))
        def _():
            down_copy(t + k).wait_send()

    for p in range(n_tensor):
        far_copy(p, b).wait_send()
        near_copy(0, p, b).wait_send()
        near_copy(1, p, far).wait_send()
        part_copy(p).wait_send()
        leave(p).wait()


def fused(axes, sizes, queries, keys, values, lengths, out_weight):
    n_seq, n_tensor, n_bucket = sizes
    rows, width = queries.shape[1:]
    group = n_seq * n_tensor
    heads = width // HS // group
    total = group * rows
    half = width // n_seq
    vmem = pl.BlockSpec(memory_space=pltpu.VMEM)
    dma = pltpu.SemaphoreType.DMA
    return pl.pallas_call(
        functools.partial(whole_kernel, axes, sizes),
        out_shape=jax.ShapeDtypeStruct(queries.shape, queries.dtype),
        in_specs=[pl.BlockSpec(memory_space=pltpu.SMEM), vmem, vmem, vmem, vmem],
        out_specs=pl.BlockSpec(memory_space=pl.ANY),
        scratch_shapes=[
            pltpu.VMEM((heads, 3, total, HS), jnp.bfloat16),
            pltpu.VMEM((heads, total, HS), jnp.bfloat16),
            pltpu.VMEM((n_seq * rows, half), jnp.bfloat16),
            pltpu.VMEM((half, width), jnp.bfloat16),
            pltpu.VMEM((rows, width), jnp.bfloat16),
            pltpu.VMEM((rows, width), jnp.bfloat16),
            pltpu.VMEM((rows, width), jnp.float32),
            dma((heads, 3, group)),
            dma((heads, 3, group)),
            dma((heads, 2, n_tensor)),
            dma((heads, 2, n_tensor)),
            dma((n_tensor,)),
            dma((n_tensor,)),
            dma((n_tensor,)),
            dma((n_tensor,)),
            dma((n_tensor,)),
            dma((2, n_tensor)),
            dma((2, n_tensor)),
            dma((n_tensor,)),
            dma((n_tensor,)),
            dma((n_tensor,)),
        ],
        compiler_params=pltpu.CompilerParams(has_side_effects=True, vmem_limit_bytes=56 * 1024 * 1024),
    )(lengths, queries, keys, values, out_weight)


def solution(mesh):
    in_specs = (
        P("bucket", ("seq", "tensor"), None),
        P("bucket", ("seq", "tensor"), None),
        P("bucket", ("seq", "tensor"), None),
        P("bucket"),
        P(("seq", "bucket"), "tensor"),
    )
    out_specs = P("bucket", ("seq", "tensor"), None)
    sizes = tuple(mesh.shape[name] for name in ("seq", "tensor", "bucket"))

    def step(queries, keys, values, lengths, out_weight):
        head_count = queries.shape[2] // HS
        fits = sizes[0] == 2 and sizes[1] == sizes[2] == 4 and head_count % (sizes[0] * sizes[1]) == 0
        if fits:
            return fused(mesh.axis_names, sizes, queries, keys, values, lengths, out_weight)
        return shards(queries, keys, values, lengths, out_weight)

    return jax.shard_map(step, mesh=mesh, in_specs=in_specs, out_specs=out_specs, check_vma=False)
```

```python
import functools
import math

import jax
import jax.numpy as jnp
from jax import lax
from jax.experimental import pallas as pl
from jax.experimental.pallas import tpu as pltpu
from jax.sharding import PartitionSpec as P

HS = 128


MASKED_SCORE = -1e30


def shards(queries, keys, values, lengths, out_weight):
    tok_rows = queries.shape[1]
    n_tensor = lax.axis_size("tensor")
    tensor_index = lax.axis_index("tensor")
    live_len = lengths[0]
    local_q, local_k, local_v = (
        lax.all_to_all(queries[0], "seq", split_axis=1, concat_axis=0, tiled=True),
        lax.all_to_all(keys[0], "seq", split_axis=1, concat_axis=0, tiled=True),
        lax.all_to_all(values[0], "seq", split_axis=1, concat_axis=0, tiled=True),
    )
    row_count, col_count = local_q.shape
    head_count = col_count // HS
    query_heads = local_q.reshape(row_count, head_count, HS)

    def spots(first_row, total_rows):
        index_row = first_row + jnp.arange(total_rows, dtype=jnp.int32)
        owner = index_row // row_count
        within = index_row % row_count
        return (within // tok_rows * n_tensor + owner) * tok_rows + within % tok_rows

    query_usable = spots(tensor_index * row_count, row_count) < live_len
    initial = (
        jnp.full((row_count, head_count), MASKED_SCORE, jnp.float32),
        jnp.zeros((row_count, head_count), jnp.float32),
        jnp.zeros((row_count, head_count, HS), jnp.float32),
    )
    carried = initial
    first_row = jnp.int32(0)
    key_rows = lax.all_gather(local_k, "tensor", axis=0, tiled=True)
    value_rows = lax.all_gather(local_v, "tensor", axis=0, tiled=True)
    for offset in range(key_rows.shape[0] // row_count):
        row_peak, row_sum, accumulated = carried
        key_tile = key_rows[offset * row_count : (offset + 1) * row_count].reshape(
            row_count, head_count, HS
        )
        value_tile = value_rows[offset * row_count : (offset + 1) * row_count].reshape(
            row_count, head_count, HS
        )
        key_usable = spots(first_row + offset * row_count, row_count) < live_len
        scores = jnp.einsum(
            "qhd,khd->qhk", query_heads, key_tile, preferred_element_type=jnp.float32
        ) * HS ** (-0.5)
        scores = jnp.where(key_usable[None, None, :], scores, MASKED_SCORE)
        peak_new = jnp.maximum(row_peak, jnp.max(scores, axis=-1))
        exponent = jnp.where(key_usable[None, None, :], jnp.exp(scores - peak_new[..., None]), 0.0)
        rescale = jnp.exp(row_peak - peak_new)
        accumulated = accumulated * rescale[..., None] + jnp.einsum(
            "qhk,khd->qhd",
            exponent.astype(jnp.bfloat16),
            value_tile,
            preferred_element_type=jnp.float32,
        )
        carried = (peak_new, row_sum * rescale + jnp.sum(exponent, axis=-1), accumulated)
    row_peak, row_sum, accumulated = carried
    attended = accumulated / row_sum[..., None]
    mixed = jnp.where(query_usable[:, None], attended.reshape(row_count, col_count), 0.0).astype(
        jnp.bfloat16
    )
    restored = lax.all_to_all(mixed, "seq", split_axis=0, concat_axis=1, tiled=True)
    wide_weight = lax.all_gather(out_weight, "tensor", axis=1, tiled=True)
    summed = jnp.dot(
        restored,
        lax.all_gather(wide_weight, ("seq", "bucket"), axis=0, tiled=True),
        preferred_element_type=jnp.float32,
    )
    return summed.astype(jnp.bfloat16)[None]


def whole_kernel(
    axes, sizes, len_ref, q_ref, k_ref, v_ref, w_ref, out_ref,
    got, done, mixed, weight, part_out, part_in, own_part,
    qkv_send, qkv_recv, att_send, att_recv, up_send, down_send, line_recv,
    far_send, far_recv, near_send, near_recv, part_send, part_recv, out_sem,
):
    n_seq, n_tensor, n_bucket = sizes
    s, t, b = lax.axis_index("seq"), lax.axis_index("tensor"), lax.axis_index("bucket")
    group = n_seq * n_tensor
    rows = q_ref.shape[1]
    width = q_ref.shape[2]
    heads = width // HS // group
    w_rows, w_cols = w_ref.shape
    block = n_seq * rows
    live = len_ref[0]

    def device(ds, dt, db):
        place = {"seq": ds, "tensor": dt, "bucket": db}
        return tuple(place[name] for name in axes)

    def remote(src, dst, send, recv, where):
        return pltpu.make_async_remote_copy(
            src_ref=src, dst_ref=dst, send_sem=send, recv_sem=recv,
            device_id=where, device_id_type=pl.DeviceIdType.MESH,
        )

    me = s * n_tensor + t
    streams = (q_ref, k_ref, v_ref)

    def spot(ds, dt):
        return pl.ds(pl.multiple_of((dt * n_seq + ds) * rows, rows), rows)

    def qkv_copy(h, j, step, peer, source):
        cols = pl.ds(pl.multiple_of((peer * heads + h) * HS, HS), HS)
        return remote(
            streams[j].at[0, :, cols],
            got.at[h, j, spot(source // n_tensor, source % n_tensor), :],
            qkv_send.at[h, j, step],
            qkv_recv.at[h, j, step],
            device(peer // n_tensor, peer % n_tensor, b),
        )

    def start_qkv(h):
        def body(step, carry):
            peer = (me + step) % group
            for j in range(3):
                qkv_copy(h, j, step, peer, me).start()
            return carry

        lax.fori_loop(1, group, body, 0)

    def piece(row_block, col_block):
        return weight.at[
            pl.ds(pl.multiple_of(row_block * w_rows, w_rows), w_rows),
            pl.ds(pl.multiple_of(col_block * w_cols, w_cols), w_cols),
        ]

    far, near = (b + 2) % 4, b + 1 - 2 * (b % 2)

    def up_copy(p):
        return remote(piece(b, p), piece(b, p), up_send.at[p], line_recv.at[p], device(s, t + 1, b))

    def down_copy(p):
        return remote(piece(b, p), piece(b, p), down_send.at[p], line_recv.at[p], device(s, t - 1, b))

    def far_copy(p, row_block):
        return remote(piece(row_block, p), piece(row_block, p), far_send.at[p], far_recv.at[p], device(s, t, far))

    def near_copy(k, p, row_block):
        return remote(
            piece(row_block, p), piece(row_block, p), near_send.at[k, p], near_recv.at[k, p], device(s, t, near)
        )

    def spread(p):
        far_copy(p, b).start()
        near_copy(0, p, b).start()

    def relay(k):
        @pl.when(t >= k)
        def _():
            up_copy(t - k).wait_recv()

            @pl.when(t < n_tensor - 1)
            def _():
                up_copy(t - k).start()

            spread(t - k)

        @pl.when(t + k < n_tensor)
        def _():
            down_copy(t + k).wait_recv()

            @pl.when(t > 0)
            def _():
                down_copy(t + k).start()

            spread(t + k)

    weight[
        pl.ds(pl.multiple_of(b * w_rows, w_rows), w_rows),
        pl.ds(pl.multiple_of(t * w_cols, w_cols), w_cols),
    ] = w_ref[...]

    @pl.when(t < n_tensor - 1)
    def _():
        up_copy(t).start()

    @pl.when(t > 0)
    def _():
        down_copy(t).start()

    start_qkv(0)
    spread(t)

    for h in range(heads):
        cols = pl.ds(pl.multiple_of((me * heads + h) * HS, HS), HS)
        for j in range(3):
            got[h, j, spot(s, t), :] = streams[j][0, :, cols]

    total = group * rows
    index = lax.broadcasted_iota(jnp.int32, (1, total), 1)
    token = (index % block // rows * n_tensor + index // block) * rows + index % rows
    usable = token < live
    factor = HS ** (-0.5) * math.log2(math.e)

    def slot_of(side):
        return (side + s) % 2

    def att_copy(h, step, target, source, side=None):
        first, count, slot = (0, block, 0) if side is None else (side * rows, rows, slot_of(side))
        here = pl.ds(pl.multiple_of(target * block + first, rows), count)
        there = pl.ds(pl.multiple_of(first, rows), count)
        cols = pl.ds(pl.multiple_of((source * heads + h) * HS, HS), HS)
        return remote(
            done.at[h, here, :], mixed.at[there, cols],
            att_send.at[h, slot, step], att_recv.at[h, slot, step], device(s, target, b),
        )

    def attend(h, target, first, count):
        here = pl.ds(pl.multiple_of(target * block + first, rows), count)
        scores = lax.dot_general(
            got[h, 0, here, :], got[h, 1], (((1,), (1,)), ((), ())), preferred_element_type=jnp.float32
        )
        scores = jnp.where(usable, scores, MASKED_SCORE)
        peak = jnp.max(scores, axis=-1, keepdims=True)
        expo = jnp.exp2((scores - peak) * factor)
        denominator = jnp.sum(expo, axis=-1, keepdims=True)
        result = jnp.dot(expo.astype(jnp.bfloat16), got[h, 2], preferred_element_type=jnp.float32) / denominator
        row = first + lax.broadcasted_iota(jnp.int32, (count, 1), 0)
        own_token = (row // rows * n_tensor + target) * rows + row % rows
        return jnp.where(own_token < live, result, 0.0).astype(jnp.bfloat16)

    def attend_all(h, first, count, side):
        def one(step, carry):
            target = (t + step) % n_tensor
            done[h, pl.ds(pl.multiple_of(target * block + first, rows), count), :] = attend(h, target, first, count)
            att_copy(h, step, target, t, side).start()
            return carry

        lax.fori_loop(1, n_tensor, one, 0)
        mixed[
            pl.ds(pl.multiple_of(first, rows), count), pl.ds(pl.multiple_of((t * heads + h) * HS, HS), HS)
        ] = attend(h, t, first, count)

    upper = t // 2
    order = (t, 1 - t + 4 * upper, 2 - upper, 3 - 3 * upper)

    def forward(p):
        far_copy(p, far).wait_recv()
        near_copy(1, p, far).start()

    for h in range(heads):
        if h == 0:
            relay(1)
            start_qkv(1)
        elif h == 1:
            relay(2)
            for later in range(2, heads):
                start_qkv(later)
        elif h == 2:
            relay(3)

        def arrive(step, carry):
            source = (me + group - step) % group
            for j in range(3):
                qkv_copy(h, j, step, me, source).wait_recv()
            return carry

        lax.fori_loop(1, group, arrive, 0)
        if 1 <= h <= 2:
            forward(order[h - 1])
        if h + 1 < heads:
            attend_all(h, 0, block, None)
        else:
            attend_all(h, (1 - s) * rows, rows, 1 - s)
            attend_all(h, s * rows, rows, s)
    for k in range(heads, 3):
        relay(k)
    for k in range(max(heads - 1, 0), 3):
        forward(order[k])

    def back(h, side):
        def body(step, carry):
            att_copy(h, step, t, (t + n_tensor - step) % n_tensor, side).wait_recv()
            return carry

        lax.fori_loop(1, n_tensor, body, 0)

    def cut_of(p):
        return pl.ds(pl.multiple_of(p * w_cols, w_cols), w_cols)

    def part_copy(p):
        cut = cut_of(p)
        return remote(
            part_out.at[:, cut], part_in.at[:, cut], part_send.at[p], part_recv.at[p], device(1 - s, t, b)
        )

    def leave(p):
        cut = cut_of(p)
        return pltpu.make_async_copy(part_in.at[:, cut], out_ref.at[0, :, cut], out_sem.at[p])

    for h in range(heads - 1):
        back(h, None)
    back(heads - 1, 1 - s)
    for k, p in enumerate(order):
        near_copy(0, p, near).wait_recv()
        near_copy(1, p, (near + 2) % 4).wait_recv()
        cut = cut_of(p)
        part_out[:, cut] = jnp.dot(
            mixed[pl.ds(pl.multiple_of((1 - s) * rows, rows), rows), :], weight[:, cut],
            preferred_element_type=jnp.float32,
        ).astype(jnp.bfloat16)
        part_copy(p).start()
        if k == 2:
            forward(order[3])
    back(heads - 1, s)
    for p in order:
        cut = cut_of(p)
        own_part[:, cut] = jnp.dot(
            mixed[pl.ds(pl.multiple_of(s * rows, rows), rows), :], weight[:, cut],
            preferred_element_type=jnp.float32,
        )
    for p in order:
        cut = cut_of(p)
        part_copy(p).wait_recv()
        part_in[:, cut] = (own_part[:, cut] + part_in[:, cut].astype(jnp.float32)).astype(jnp.bfloat16)
        leave(p).start()

    for h in range(heads):
        def sent(step, carry):
            peer = (me + step) % group
            for j in range(3):
                qkv_copy(h, j, step, peer, me).wait_send()
            return carry

        lax.fori_loop(1, group, sent, 0)

        def att_sent(step, carry):
            if h + 1 < heads:
                att_copy(h, step, (t + step) % n_tensor, t).wait_send()
            else:
                att_copy(h, step, (t + step) % n_tensor, t, 1 - s).wait_send()
                att_copy(h, step, (t + step) % n_tensor, t, s).wait_send()
            return carry

        lax.fori_loop(1, n_tensor, att_sent, 0)
    for k in range(n_tensor):
        @pl.when((t >= k) & (t < n_tensor - 1))
        def _():
            up_copy(t - k).wait_send()

        @pl.when((t + k < n_tensor) & (t > 0))
        def _():
            down_copy(t + k).wait_send()

    for p in range(n_tensor):
        far_copy(p, b).wait_send()
        near_copy(0, p, b).wait_send()
        near_copy(1, p, far).wait_send()
        part_copy(p).wait_send()
        leave(p).wait()


def fused(axes, sizes, queries, keys, values, lengths, out_weight):
    n_seq, n_tensor, n_bucket = sizes
    rows, width = queries.shape[1:]
    group = n_seq * n_tensor
    heads = width // HS // group
    total = group * rows
    half = width // n_seq
    vmem = pl.BlockSpec(memory_space=pltpu.VMEM)
    dma = pltpu.SemaphoreType.DMA
    return pl.pallas_call(
        functools.partial(whole_kernel, axes, sizes),
        out_shape=jax.ShapeDtypeStruct(queries.shape, queries.dtype),
        in_specs=[pl.BlockSpec(memory_space=pltpu.SMEM), vmem, vmem, vmem, vmem],
        out_specs=pl.BlockSpec(memory_space=pl.ANY),
        scratch_shapes=[
            pltpu.VMEM((heads, 3, total, HS), jnp.bfloat16),
            pltpu.VMEM((heads, total, HS), jnp.bfloat16),
            pltpu.VMEM((n_seq * rows, half), jnp.bfloat16),
            pltpu.VMEM((half, width), jnp.bfloat16),
            pltpu.VMEM((rows, width), jnp.bfloat16),
            pltpu.VMEM((rows, width), jnp.bfloat16),
            pltpu.VMEM((rows, width), jnp.float32),
            dma((heads, 3, group)),
            dma((heads, 3, group)),
            dma((heads, 2, n_tensor)),
            dma((heads, 2, n_tensor)),
            dma((n_tensor,)),
            dma((n_tensor,)),
            dma((n_tensor,)),
            dma((n_tensor,)),
            dma((n_tensor,)),
            dma((2, n_tensor)),
            dma((2, n_tensor)),
            dma((n_tensor,)),
            dma((n_tensor,)),
            dma((n_tensor,)),
        ],
        compiler_params=pltpu.CompilerParams(has_side_effects=True, vmem_limit_bytes=56 * 1024 * 1024),
    )(lengths, queries, keys, values, out_weight)


def solution(mesh):
    in_specs = (
        P("bucket", ("seq", "tensor"), None),
        P("bucket", ("seq", "tensor"), None),
        P("bucket", ("seq", "tensor"), None),
        P("bucket"),
        P(("seq", "bucket"), "tensor"),
    )
    out_specs = P("bucket", ("seq", "tensor"), None)
    sizes = tuple(mesh.shape[name] for name in ("seq", "tensor", "bucket"))

    def step(queries, keys, values, lengths, out_weight):
        head_count = queries.shape[2] // HS
        fits = sizes[0] == 2 and sizes[1] == sizes[2] == 4 and head_count % (sizes[0] * sizes[1]) == 0
        if fits:
            return fused(mesh.axis_names, sizes, queries, keys, values, lengths, out_weight)
        return shards(queries, keys, values, lengths, out_weight)

    return jax.shard_map(step, mesh=mesh, in_specs=in_specs, out_specs=out_specs, check_vma=False)
```
